32 devices in a mesh: seq: 8 (over y, x, core), kvh: 4 (over z).
Axes of the slice: x: 2, y: 2, z: 4, core: 2. Of those that a mesh axis runs over, the one named last changes fastest.
Arguments:
- queries: bfloat16 [64, 32, 128], P(('seq', 'kvh')), may hold values from -9 to 9
- attn_out: bfloat16 [64, 32, 128], P(('seq', 'kvh')), may hold values from -0.59765625 to 0.59765625
- grad_out: bfloat16 [64, 32, 128], P(('seq', 'kvh')), may hold values from -384 to 384
- log_norms: float32 [64, 32], P(('seq', 'kvh')), may hold values from 0 to 14, as said below
- query_starts: int32 [64], replicated, may hold values from 0 to 2048
- keys: bfloat16 [8192, 4, 128], P('seq', 'kvh'), may hold values from -6 to 6
- values: bfloat16 [8192, 4, 128], P('seq', 'kvh'), may hold values from -6 to 6
Outputs:
- grad_query: bfloat16 [64, 32, 128], P(('seq', 'kvh'))
- grad_keys: bfloat16 [8192, 4, 128], P('seq', 'kvh')
- grad_values: bfloat16 [8192, 4, 128], P('seq', 'kvh')
The draws below stay inside these ranges and needn't reach their ends.
Inputs may be any that keep to these rules, and one draw needn't show every extreme that they name: `log_norms`: each entry lies within one of the log of its token's number of visible positions plus 1.125.
All inputs are finite; a program needn't handle non-finite values.
Results may differ from the reference program's by a relative error of at most 0.0052.
Values may be sent and summed in bfloat16 or wider, within the bound.
No kernel may reach another device: no remote copies, remote signals or barrier semaphores. Data moves between devices by JAX's collectives and lax.ppermute only.
A program may use at most 64 MiB of HBM per device.

```python
import jax
import jax.numpy as jnp
from jax import lax

HD = 128
GROUP = 8
KEY_DEV = 1024
KVH = 4
H = 32
CTX = 8192
Q_TOK = 64
N_SEQ = 8


def first_positions(key):
    highest = CTX // 4
    starts = jax.random.randint(jax.random.fold_in(key, 5), (Q_TOK,), 0, highest + 1, dtype=jnp.int32)
    order = jax.random.permutation(jax.random.fold_in(key, 7), Q_TOK)
    places = jnp.arange(Q_TOK, dtype=jnp.int32)
    starts = jnp.where(places == order[0], 0, starts)
    starts = jnp.where(places == order[1], highest, starts)
    return starts.astype(jnp.int32)


def draw_query_starts(key, part):
    return first_positions(key)


def draw_log_norms(key, part):
    firsts = first_positions(key)
    position = CTX - Q_TOK + jnp.arange(Q_TOK, dtype=jnp.int32)
    counts = (position - firsts + 1).astype(jnp.float32)
    baseline = jnp.log(counts) + 1.125
    jitter = jnp.clip(0.3 * jax.random.normal(jax.random.fold_in(key, 11), (Q_TOK, H), jnp.float32), -1.0, 1.0)
    return baseline[:, None] + jitter


def shard_levels(stream_key, shape, shards, smallest, high):
    loudness, own = 1.0, jax.random.fold_in(stream_key, 6)
    for axis_at, parts in shards:
        heights = jnp.exp(jax.random.uniform(jax.random.fold_in(own, axis_at), (parts,), jnp.float32, smallest / len(shards), high / len(shards)))
        loudness = loudness * jnp.repeat(heights, shape[axis_at] // parts).reshape([-1 if axis == axis_at else 1 for axis in range(len(shape))])
    return loudness


def gaussian(own_key, extent, spread, bound, split=(), kind=jnp.bfloat16):
    array = spread * jax.random.normal(own_key, extent, jnp.float32)
    if split:
        array = array * shard_levels(own_key, extent, split, -0.22, 0.18)
    return jnp.clip(array, -bound, bound).astype(kind)


def setup_inputs(seed: int = 0) -> dict:
    key_of = jax.random.split(jax.random.key(seed), 8)
    queries = gaussian(key_of[0], (Q_TOK, H, HD), 1.5, 9.0, ((0, 32),))
    attn_out = gaussian(key_of[1], (Q_TOK, H, HD), 0.1, 0.59765625, ((0, 32),))
    grad_out = gaussian(key_of[2], (Q_TOK, H, HD), 64.0, 384.0, ((0, 32),))
    log_norms = draw_log_norms(jax.random.fold_in(key_of[7], 71), 0)
    query_starts = draw_query_starts(jax.random.fold_in(key_of[7], 71), 0)
    keys = gaussian(key_of[5], (CTX, KVH, HD), 1.0, 6.0, ((0, 8), (1, 4)))
    values = gaussian(key_of[6], (CTX, KVH, HD), 1.0, 6.0, ((0, 8), (1, 4)))
    return {"queries": queries, "attn_out": attn_out, "grad_out": grad_out, "log_norms": log_norms, "query_starts": query_starts, "keys": keys, "values": values}


def reference(queries, attn_out, grad_out, log_norms, query_starts, keys, values):
    scaling = HD ** -0.5
    deltas = jnp.sum(grad_out.astype(jnp.float32) * attn_out.astype(jnp.float32), axis=-1)
    query_wide = queries.astype(jnp.float32).reshape(Q_TOK, KVH, GROUP, HD)
    grad_wide = grad_out.astype(jnp.float32).reshape(Q_TOK, KVH, GROUP, HD)
    norm_grid = log_norms.reshape(Q_TOK, KVH, GROUP)
    delta_grid = deltas.reshape(Q_TOK, KVH, GROUP)
    query_pos = CTX - Q_TOK + jnp.arange(Q_TOK, dtype=jnp.int32)
    key_blocks = keys.reshape(N_SEQ, KEY_DEV, KVH, HD)
    value_blocks = values.reshape(N_SEQ, KEY_DEV, KVH, HD)

    def visit_owner(grad_query, inputs):
        block_index, key_block, value_block = inputs
        key_pos = block_index * KEY_DEV + jnp.arange(KEY_DEV, dtype=jnp.int32)
        visible = (key_pos[None, :] >= query_starts[:, None]) & (key_pos[None, :] <= query_pos[:, None])
        key_wide = key_block.astype(jnp.float32)
        value_wide = value_block.astype(jnp.float32)
        scores = jnp.einsum("qngd,knd->qngk", query_wide, key_wide) * scaling
        weights = jnp.where(visible[:, None, None, :], jnp.exp(scores - norm_grid[..., None]), 0.0)
        weight_grad = jnp.einsum("qngd,knd->qngk", grad_wide, value_wide)
        score_grad = weights * (weight_grad - delta_grid[..., None])
        weight_half = lax.optimization_barrier(weights.astype(jnp.bfloat16)).astype(jnp.float32)
        score_half = lax.optimization_barrier(score_grad.astype(jnp.bfloat16)).astype(jnp.float32)
        value_grad = jnp.einsum("qngk,qngd->knd", weight_half, grad_wide)
        key_grad = jnp.einsum("qngk,qngd->knd", score_half, query_wide) * scaling
        grad_query = grad_query + jnp.einsum("qngk,knd->qngd", score_half, key_wide) * scaling
        return grad_query, (key_grad.astype(jnp.bfloat16), value_grad.astype(jnp.bfloat16))

    initial = jnp.zeros((Q_TOK, KVH, GROUP, HD), jnp.float32)
    indices = jnp.arange(N_SEQ, dtype=jnp.int32)
    grad_query, (key_grads, value_grads) = lax.scan(visit_owner, initial, (indices, key_blocks, value_blocks))
    return (grad_query.reshape(Q_TOK, H, HD).astype(jnp.bfloat16),
            key_grads.reshape(CTX, KVH, HD),
            value_grads.reshape(CTX, KVH, HD))
```

```python
import functools
import math

import jax
import jax.numpy as jnp
from jax import lax
from jax.experimental import pallas as pl
from jax.experimental.pallas import tpu as pltpu
from jax.sharding import PartitionSpec as P

LANES = 128
PARTS = 3
BF = jnp.bfloat16
F32 = jnp.float32
VM = pl.BlockSpec(memory_space=pltpu.VMEM)


def split_parts(value):
    out = []
    for _ in range(PARTS):
        part = value.astype(BF)
        out.append(part)
        value = value - part.astype(F32)
    return out


def prep_body(q_ref, g_ref, o_ref, n_ref, out_ref, *, root):
    tokens, heads, _ = q_ref.shape
    seqs, kvs, rows, _ = out_ref.shape
    group = heads // kvs
    block = tokens * group
    stride = LANES // tokens
    lane = lax.broadcasted_iota(jnp.int32, (heads, LANES), 1)
    extra = jnp.zeros((heads, LANES), F32)
    pick = lax.broadcasted_iota(jnp.int32, (heads, heads), 0) == lax.broadcasted_iota(
        jnp.int32, (heads, heads), 1
    )
    for t in range(tokens):
        g = g_ref[t].astype(F32)
        o = o_ref[t].astype(F32)
        delta = jnp.sum(g * o, axis=-1, keepdims=True)
        norm_row = jnp.broadcast_to(n_ref[t : t + 1, :], (heads, heads))
        norm = jnp.sum(jnp.where(pick, norm_row, 0.0), axis=-1, keepdims=True) * root
        for p, part in enumerate(split_parts(norm) + split_parts(delta)):
            extra = jnp.where(lane == t * stride + p, part.astype(F32), extra)
    extra = extra.astype(BF)
    for k in range(kvs):
        part = slice(k * group, (k + 1) * group)
        for s in range(seqs):
            for t in range(tokens):
                out_ref[s, k, t * group : (t + 1) * group, :] = q_ref[t, part, :]
                out_ref[s, k, block + t * group : block + (t + 1) * group, :] = g_ref[t, part, :]
            out_ref[s, k, 2 * block : rows, :] = extra[part, :]


def unpack(m_ref, first, count, tokens, group):
    block = tokens * group
    stride = LANES // tokens
    q = m_ref[pl.ds(first, count), 0:block, :].reshape(count * block, LANES)
    g = m_ref[pl.ds(first, count), block : 2 * block, :].reshape(count * block, LANES)
    e = m_ref[pl.ds(first, count), 2 * block : 2 * block + group, :]
    lane = lax.broadcasted_iota(jnp.int32, (count, group, LANES), 2)
    pieces = [jnp.where((lane >= t * stride) & (lane < (t + 1) * stride), e, jnp.zeros_like(e)) for t in range(tokens)]
    extra = jnp.stack(pieces, axis=1).reshape(count * block, LANES)
    return q, g, extra


def grads_body(m_ref, k_ref, v_ref, lo_ref, hi_ref, w_ref, s_ref, dq_ref, *, tokens, group, step, scaling):
    messages = m_ref.shape[0]
    keys = k_ref.shape[0]
    block = tokens * group
    stride = LANES // tokens
    lane = lax.broadcasted_iota(jnp.int32, (keys, LANES), 1) % stride
    minus = jnp.full((keys, LANES), -1.0, F32)
    norm_cols = jnp.where(lane < PARTS, minus, 0.0).astype(BF)
    delta_cols = jnp.where((lane >= PARTS) & (lane < 2 * PARTS), minus, 0.0).astype(BF)
    k_wide = jnp.concatenate([k_ref[...], norm_cols], axis=1)
    v_wide = jnp.concatenate([v_ref[...], delta_cols], axis=1)
    factor = scaling * math.log2(math.e)
    nt = (((1,), (1,)), ((), ()))
    rows = step * block

    def visit(at):
        first = pl.ds(at * rows, rows)
        q, g, extra = unpack(m_ref, at * step, step, tokens, group)
        scores = lax.dot_general(jnp.concatenate([q, extra], axis=1), k_wide, nt, preferred_element_type=F32)
        pos = lax.broadcasted_iota(jnp.int32, (rows, keys), 1)
        lo = jnp.tile(lo_ref[first, :], (1, keys // LANES))
        hi = jnp.tile(hi_ref[first, :], (1, keys // LANES))
        weights = jnp.where((pos >= lo) & (pos <= hi), jnp.exp2(scores * factor), 0.0)
        pulled = lax.dot_general(jnp.concatenate([g, extra], axis=1), v_wide, nt, preferred_element_type=F32)
        s_half = (weights * pulled).astype(BF)
        w_ref[first, :] = weights.astype(BF)
        s_ref[first, :] = s_half
        dq = jnp.dot(s_half, k_ref[...], preferred_element_type=F32) * scaling
        dq_ref[pl.ds(at * step, step)] = dq.astype(BF).reshape(step, block, LANES)

    if messages // step <= 4:
        for at in range(messages // step):
            visit(at)
    else:

        @pl.loop(0, messages // step)
        def _(at):
            visit(at)


def context_body(m_ref, w_ref, s_ref, dk_ref, dv_ref, *, tokens, group, step, scaling):
    messages = m_ref.shape[0]
    block = tokens * group
    rows = step * block
    tn = (((0,), (0,)), ((), ()))
    keys = w_ref.shape[1]

    def visit(at, sums):
        first = pl.ds(at * rows, rows)
        q = m_ref[pl.ds(at * step, step), 0:block, :].reshape(rows, LANES)
        g = m_ref[pl.ds(at * step, step), block : 2 * block, :].reshape(rows, LANES)
        dk = lax.dot_general(s_ref[first, :], q, tn, preferred_element_type=F32)
        dv = lax.dot_general(w_ref[first, :], g, tn, preferred_element_type=F32)
        return (sums[0] + dk, sums[1] + dv)

    zero = jnp.zeros((keys, LANES), F32)
    if messages // step == 1:
        sums = visit(0, (zero, zero))
    else:
        sums = lax.fori_loop(0, messages // step, visit, (zero, zero))
    dk_ref[...] = (sums[0] * scaling).astype(BF)
    dv_ref[...] = sums[1].astype(BF)


def local(queries, attn_out, grad_out, log_norms, query_starts, keys, values):
    scaling = queries.shape[-1] ** (-0.5)
    seqs, kvs = lax.axis_size("seq"), lax.axis_size("kvh")
    peers = seqs * kvs
    tokens, heads, width = queries.shape
    group = heads // kvs
    block = tokens * group
    rows = peers * block
    both = ("seq", "kvh")
    message = pl.pallas_call(
        functools.partial(prep_body, root=1.0 / scaling),
        out_shape=jax.ShapeDtypeStruct((seqs, kvs, 2 * block + group, width), BF),
        in_specs=[VM] * 4,
        out_specs=VM,
        name="prep",
    )(queries, grad_out, attn_out, log_norms)
    message = message.reshape(peers, 2 * block + group, width)
    got = lax.all_to_all(message, both, split_axis=0, concat_axis=0, tiled=True)

    key_count = keys.shape[0]
    base = lax.axis_index("seq") * key_count
    all_tokens = query_starts.shape[0]
    last = seqs * key_count - all_tokens + jnp.arange(all_tokens, dtype=jnp.int32) - base
    spread = lambda x: jnp.broadcast_to(jnp.repeat(x, group)[:, None], (rows, LANES))
    lo, hi = spread(query_starts - base), spread(last)
    key_rows, value_rows = keys[:, 0, :], values[:, 0, :]
    step = min(peers, 8)
    weights, score_grads, partial = pl.pallas_call(
        functools.partial(grads_body, tokens=tokens, group=group, step=step, scaling=scaling),
        out_shape=(
            jax.ShapeDtypeStruct((rows, key_count), BF),
            jax.ShapeDtypeStruct((rows, key_count), BF),
            jax.ShapeDtypeStruct((peers, block, width), BF),
        ),
        in_specs=[VM] * 5,
        out_specs=(VM, VM, VM),
        name="grads",
    )(got, key_rows, value_rows, lo, hi)
    back = lax.all_to_all(partial, both, split_axis=0, concat_axis=0, tiled=True)
    grad_keys, grad_values = pl.pallas_call(
        functools.partial(context_body, tokens=tokens, group=group, step=min(peers, 32), scaling=scaling),
        out_shape=(jax.ShapeDtypeStruct((key_count, width), BF),) * 2,
        in_specs=[VM] * 3,
        out_specs=(VM, VM),
        name="context",
    )(got, weights, score_grads)
    back = back.reshape(seqs, kvs, tokens, group, width).astype(F32)
    grad_query = jnp.sum(back, axis=0).transpose(1, 0, 2, 3).reshape(tokens, heads, width).astype(BF)
    return (grad_query, grad_keys[:, None, :], grad_values[:, None, :])


def solution(mesh):
    return jax.shard_map(
        local,
        mesh=mesh,
        in_specs=(
            P(("seq", "kvh"), None, None),
            P(("seq", "kvh"), None, None),
            P(("seq", "kvh"), None, None),
            P(("seq", "kvh"), None),
            P(),
            P("seq", "kvh", None),
            P("seq", "kvh", None),
        ),
        out_specs=(P(("seq", "kvh"), None, None), P("seq", "kvh", None), P("seq", "kvh", None)),
        check_vma=False,
    )
```

```python
import functools
import math

import jax
import jax.numpy as jnp
from jax import lax
from jax.experimental import pallas as pl
from jax.experimental.pallas import tpu as pltpu
from jax.sharding import PartitionSpec as P

LANES = 128
PARTS = 3
BF = jnp.bfloat16
F32 = jnp.float32
VM = pl.BlockSpec(memory_space=pltpu.VMEM)
ANY = pl.BlockSpec(memory_space=pl.ANY)


SMALL = 1 << 20


def held(shape, dtype=BF):
    if math.prod(shape) * jnp.dtype(dtype).itemsize <= SMALL:
        return pltpu.VMEM(shape, dtype)
    return jax.ShapeDtypeStruct(shape, dtype)


def fast(value):
    if value.size * value.dtype.itemsize <= SMALL:
        return pltpu.with_memory_space_constraint(value, pltpu.VMEM)
    return value


def kernel(body, mib, **kwargs):
    return pl.pallas_call(body, compiler_params=pltpu.CompilerParams(vmem_limit_bytes=mib << 20), **kwargs)


def split_parts(value):
    out = []
    for _ in range(PARTS):
        part = value.astype(BF)
        out.append(part)
        value = value - part.astype(F32)
    return out


def prep_body(q_hbm, g_hbm, o_hbm, n_hbm, out_hbm, q_ref, g_ref, o_ref, n_ref, m_ref, in_sems, out_sems, *, root):
    tokens, heads, _ = q_ref.shape
    seqs = out_hbm.shape[0]
    kvs, rows, _ = m_ref.shape
    group = heads // kvs
    block = tokens * group
    stride = LANES // tokens
    loads = [
        pltpu.make_async_copy(src, dst, in_sems.at[i])
        for i, (src, dst) in enumerate(((n_hbm, n_ref), (g_hbm, g_ref), (o_hbm, o_ref), (q_hbm, q_ref)))
    ]
    for load in loads:
        load.start()
    lane = lax.broadcasted_iota(jnp.int32, (heads, LANES), 1)
    extra = jnp.zeros((heads, LANES), F32)
    pick = lax.broadcasted_iota(jnp.int32, (heads, heads), 0) == lax.broadcasted_iota(
        jnp.int32, (heads, heads), 1
    )
    for load in loads:
        load.wait()
    for t in range(tokens):
        g = g_ref[t].astype(F32)
        o = o_ref[t].astype(F32)
        delta = jnp.sum(g * o, axis=-1, keepdims=True)
        norm_row = jnp.broadcast_to(n_ref[t : t + 1, :], (heads, heads))
        norm = jnp.sum(jnp.where(pick, norm_row, 0.0), axis=-1, keepdims=True) * root
        for p, part in enumerate(split_parts(norm) + split_parts(delta)):
            extra = jnp.where(lane == t * stride + p, part.astype(F32), extra)
    extra = extra.astype(BF)
    for k in range(kvs):
        part = slice(k * group, (k + 1) * group)
        for t in range(tokens):
            m_ref[k, t * group : (t + 1) * group, :] = q_ref[t, part, :]
            m_ref[k, block + t * group : block + (t + 1) * group, :] = g_ref[t, part, :]
        m_ref[k, 2 * block : rows, :] = extra[part, :]
    stores = [pltpu.make_async_copy(m_ref, out_hbm.at[s], out_sems.at[s]) for s in range(seqs)]
    for store in stores:
        store.start()
    for store in stores:
        store.wait()


def unpack(m_ref, first, count, tokens, group):
    block = tokens * group
    stride = LANES // tokens
    q = m_ref[pl.ds(first, count), 0:block, :].reshape(count * block, LANES)
    g = m_ref[pl.ds(first, count), block : 2 * block, :].reshape(count * block, LANES)
    e = m_ref[pl.ds(first, count), 2 * block : 2 * block + group, :]
    lane = lax.broadcasted_iota(jnp.int32, (count, group, LANES), 2)
    pieces = [jnp.where((lane >= t * stride) & (lane < (t + 1) * stride), e, jnp.zeros_like(e)) for t in range(tokens)]
    extra = jnp.stack(pieces, axis=1).reshape(count * block, LANES)
    return q, g, extra


def stage_body(k_ref, v_ref, starts_ref, k_out, v_out, lo_ref, hi_ref, *, tokens, chips, cores, kvs):
    keys = k_ref.shape[0]
    stride = LANES // tokens
    lane = lax.broadcasted_iota(jnp.int32, (keys, LANES), 1) % stride
    minus = jnp.full((keys, LANES), -1.0, F32)
    k_out[:, 0:LANES] = k_ref[...]
    k_out[:, LANES:] = jnp.where(lane < PARTS, minus, 0.0).astype(BF)
    v_out[:, 0:LANES] = v_ref[...]
    v_out[:, LANES:] = jnp.where((lane >= PARTS) & (lane < 2 * PARTS), minus, 0.0).astype(BF)
    core = lax.axis_index("core")
    base = (lax.axis_index("chip") * cores + core) * keys
    each = kvs * tokens
    offset = chips * cores * (keys - each) - base

    def bounds(chip):
        for c in range(cores):
            first = (chip * cores + lax.rem(core + c, cores)) * each
            for t in range(each):
                row = pl.ds(chip * each + t, 1)
                lo_ref[c, row, :] = jnp.full((1, LANES), starts_ref[first + t] - base, jnp.int32)
                hi_ref[c, row, :] = jnp.full((1, LANES), offset + first + t, jnp.int32)

    if chips <= 4:
        for chip in range(chips):
            bounds(chip)
    else:
        pl.loop(0, chips)(bounds)


def grads_body(m_ref, k_ref, v_ref, lo_ref, hi_ref, *rest, tokens, group, step, scaling, turn, last):
    if last:
        done, (w_ref, s_ref, dq_hbm, dq_ref, sems) = rest[:-5], rest[-5:]
    else:
        done, (w_ref, s_ref, dq_ref) = rest[:-3], rest[-3:]
    messages = m_ref.shape[0]
    keys = k_ref.shape[0]
    block = tokens * group
    factor = scaling * math.log2(math.e)
    nt = (((1,), (1,)), ((), ()))
    rows = step * block
    here = step * tokens
    if last:
        cores = dq_hbm.shape[1]
        core = lax.axis_index("core")

        def store(c, src):
            return pltpu.make_async_copy(src, dq_hbm.at[:, lax.rem(core + c, cores)], sems.at[c])

        for c, ref in enumerate(done):
            store(c, ref).start()

    def wide_bounds(ref, at):
        each = [jnp.broadcast_to(ref[turn, pl.ds(at * here + t, 1), :], (group, LANES)) for t in range(here)]
        return jnp.tile(jnp.concatenate(each, axis=0), (1, keys // LANES))

    def visit(at):
        first = pl.ds(at * rows, rows)
        q, g, extra = unpack(m_ref, at * step, step, tokens, group)
        scores = lax.dot_general(jnp.concatenate([q, extra], axis=1), k_ref[...], nt, preferred_element_type=F32)
        pos = lax.broadcasted_iota(jnp.int32, (rows, keys), 1)
        lo, hi = wide_bounds(lo_ref, at), wide_bounds(hi_ref, at)
        weights = jnp.where((pos >= lo) & (pos <= hi), jnp.exp2(scores * factor), 0.0)
        pulled = lax.dot_general(jnp.concatenate([g, extra], axis=1), v_ref[...], nt, preferred_element_type=F32)
        s_half = (weights * pulled).astype(BF)
        w_ref[first, :] = weights.astype(BF)
        s_ref[first, :] = s_half
        dq = jnp.dot(s_half, k_ref[:, 0:LANES], preferred_element_type=F32) * scaling
        dq = dq.astype(BF).reshape(step, block, LANES)
        kvs = dq_ref.shape[1]
        for i in range(step):
            dq_ref[(at * step + i) // kvs, (at * step + i) % kvs] = dq[i]

    steps = messages // step
    if steps <= 4:
        for at in range(steps):
            visit(at)
    else:
        pl.loop(0, steps)(visit)
    if last:
        store(turn, dq_ref).start()
        for c in range(turn):
            store(c, done[c]).wait()
        store(turn, dq_ref).wait()


def context_body(*refs, tokens, group, step, scaling):
    dk_ref, dv_ref = refs[-2:]
    block = tokens * group
    tn = (((0,), (0,)), ((), ()))
    keys = dk_ref.shape[0]
    rows = step * block
    sums = (jnp.zeros((keys, LANES), F32),) * 2
    for m_ref, w_ref, s_ref in zip(refs[0:-2:3], refs[1:-2:3], refs[2:-2:3], strict=True):

        def visit(at, sums):
            first = pl.ds(at * rows, rows)
            q = m_ref[pl.ds(at * step, step), 0:block, :].reshape(rows, LANES)
            g = m_ref[pl.ds(at * step, step), block : 2 * block, :].reshape(rows, LANES)
            dk = lax.dot_general(s_ref[first, :], q, tn, preferred_element_type=F32)
            dv = lax.dot_general(w_ref[first, :], g, tn, preferred_element_type=F32)
            return (sums[0] + dk, sums[1] + dv)

        steps = m_ref.shape[0] // step
        sums = visit(0, sums) if steps == 1 else lax.fori_loop(0, steps, visit, sums)
    dk_ref[...] = (sums[0] * scaling).astype(BF)
    dv_ref[...] = sums[1].astype(BF)


def combine_body(b_ref, dq_ref):
    seqs, kvs, tokens, group, _ = b_ref.shape
    for k in range(kvs):
        for t in range(tokens):
            total = b_ref[0, k, t].astype(F32)
            for s in range(1, seqs):
                total = total + b_ref[s, k, t].astype(F32)
            dq_ref[t, k * group : (k + 1) * group, :] = total.astype(BF)


def local(queries, attn_out, grad_out, log_norms, query_starts, keys, values):
    scaling = queries.shape[-1] ** (-0.5)
    chips, cores, kvs = lax.axis_size("chip"), lax.axis_size("core"), lax.axis_size("kvh")
    senders = chips * kvs
    peers = senders * cores
    tokens, heads, width = queries.shape
    group = heads // kvs
    block = tokens * group
    rows = senders * block
    slow = lambda value: pltpu.with_memory_space_constraint(value, pltpu.HBM)
    rows_sent = 2 * block + group
    message = kernel(
        functools.partial(prep_body, root=1.0 / scaling),
        8,
        out_shape=pltpu.HBM((chips, kvs, rows_sent, width), BF),
        in_specs=[ANY] * 4,
        out_specs=ANY,
        scratch_shapes=[
            pltpu.VMEM(queries.shape, BF),
            pltpu.VMEM(queries.shape, BF),
            pltpu.VMEM(queries.shape, BF),
            pltpu.VMEM(log_norms.shape, F32),
            pltpu.VMEM((kvs, rows_sent, width), BF),
            pltpu.SemaphoreType.DMA((4,)),
            pltpu.SemaphoreType.DMA((chips,)),
        ],
        name="prep",
    )(slow(queries), slow(grad_out), slow(attn_out), slow(log_norms))
    message = message.reshape(senders, rows_sent, width)
    own = lax.all_to_all(message, ("chip", "kvh"), split_axis=0, concat_axis=0, tiled=True)
    key_count = keys.shape[0]
    here = senders * tokens
    k_wide, v_wide, lo, hi = kernel(
        functools.partial(stage_body, tokens=tokens, chips=chips, cores=cores, kvs=kvs),
        8,
        out_shape=(
            held((key_count, 2 * LANES)),
            held((key_count, 2 * LANES)),
            held((cores, here, LANES), jnp.int32),
            held((cores, here, LANES), jnp.int32),
        ),
        in_specs=[VM, VM, pl.BlockSpec(memory_space=pltpu.SMEM)],
        out_specs=(VM,) * 4,
        name="stage",
    )(keys[:, 0, :], values[:, 0, :], slow(query_starts))
    own, k_wide, v_wide, lo, hi = lax.optimization_barrier((own, k_wide, v_wide, lo, hi))
    got = [own]
    for c in range(1, cores):
        got.append(lax.ppermute(own, "core", [((i + c) % cores, i) for i in range(cores)]))
    step = math.gcd(senders, 8)
    partials, context = [], []
    for turn in range(cores):
        last = turn == cores - 1
        scratch = [pltpu.VMEM((chips, kvs, block, width), BF), pltpu.SemaphoreType.DMA((cores,))]
        w, s, partial = kernel(
            functools.partial(
                grads_body, tokens=tokens, group=group, step=step, scaling=scaling, turn=turn, last=last
            ),
            48,
            out_shape=(
                held((rows, key_count)),
                held((rows, key_count)),
                pltpu.HBM((chips, cores, kvs, block, width), BF) if last else held((chips, kvs, block, width)),
            ),
            in_specs=[VM] * (5 + turn),
            out_specs=(VM, VM, ANY if last else VM),
            scratch_shapes=scratch if last else [],
            name=f"grads{turn}",
        )(fast(got[turn]), fast(k_wide), fast(v_wide), fast(lo), fast(hi), *map(fast, partials))
        partials.append(partial)
        context += [fast(got[turn]), fast(w), fast(s)]
    partial = partials[-1].reshape(peers, block, width)
    back = lax.all_to_all(partial, ("chip", "core", "kvh"), split_axis=0, concat_axis=0, tiled=True)
    grad_keys, grad_values = kernel(
        functools.partial(context_body, tokens=tokens, group=group, step=math.gcd(senders, 16), scaling=scaling),
        48,
        out_shape=(jax.ShapeDtypeStruct((key_count, width), BF),) * 2,
        in_specs=[VM] * len(context),
        out_specs=(VM, VM),
        name="context",
    )(*context)
    grad_query = kernel(
        combine_body,
        8,
        out_shape=jax.ShapeDtypeStruct((tokens, heads, width), BF),
        in_specs=[VM],
        out_specs=VM,
        name="combine",
    )(fast(back.reshape(chips * cores, kvs, tokens, group, width)))
    return (grad_query, grad_keys[:, None, :], grad_values[:, None, :])


def solution(mesh):
    seqs, kvs = mesh.shape["seq"], mesh.shape["kvh"]
    cores = 2 if seqs % 2 == 0 else 1
    split = jax.sharding.Mesh(mesh.devices.reshape(seqs // cores, cores, kvs), ("chip", "core", "kvh"))
    token, context = ("chip", "core", "kvh"), ("chip", "core")
    return jax.shard_map(
        local,
        mesh=split,
        in_specs=(
            P(token, None, None),
            P(token, None, None),
            P(token, None, None),
            P(token, None),
            P(),
            P(context, "kvh", None),
            P(context, "kvh", None),
        ),
        out_specs=(P(token, None, None), P(context, "kvh", None), P(context, "kvh", None)),
        check_vma=False,
    )
```

```python
import functools
import math

import jax
import jax.numpy as jnp
from jax import lax
from jax.experimental import pallas as pl
from jax.experimental.pallas import tpu as pltpu
from jax.sharding import PartitionSpec as P

LANES = 128
PARTS = 3
STEP = 16
SPAN = 1024
BF = jnp.bfloat16
F32 = jnp.float32
VM = pl.BlockSpec(memory_space=pltpu.VMEM)
ANY = pl.BlockSpec(memory_space=pl.ANY)


SMALL = 1 << 20


def held(shape, dtype=BF):
    if math.prod(shape) * jnp.dtype(dtype).itemsize <= SMALL:
        return pltpu.VMEM(shape, dtype)
    return jax.ShapeDtypeStruct(shape, dtype)


def fast(value):
    if value.size * value.dtype.itemsize <= SMALL:
        return pltpu.with_memory_space_constraint(value, pltpu.VMEM)
    return value


def kernel(body, mib, **kwargs):
    return pl.pallas_call(body, compiler_params=pltpu.CompilerParams(vmem_limit_bytes=mib << 20), **kwargs)


def split_parts(value):
    out = []
    for _ in range(PARTS):
        part = value.astype(BF)
        out.append(part)
        value = value - part.astype(F32)
    return out


def prep_body(q_hbm, g_hbm, o_hbm, n_hbm, out_hbm, q_ref, g_ref, o_ref, n_ref, m_ref, in_sems, out_sems, *, root):
    tokens, heads, _ = q_ref.shape
    seqs = out_hbm.shape[0]
    kvs, rows, _ = m_ref.shape
    group = heads // kvs
    block = tokens * group
    stride = LANES // tokens
    loads = [
        pltpu.make_async_copy(src, dst, in_sems.at[i])
        for i, (src, dst) in enumerate(((n_hbm, n_ref), (g_hbm, g_ref), (o_hbm, o_ref), (q_hbm, q_ref)))
    ]
    for load in loads:
        load.start()
    lane = lax.broadcasted_iota(jnp.int32, (heads, LANES), 1)
    extra = jnp.zeros((heads, LANES), F32)
    pick = lax.broadcasted_iota(jnp.int32, (heads, heads), 0) == lax.broadcasted_iota(
        jnp.int32, (heads, heads), 1
    )
    for load in loads:
        load.wait()
    for t in range(tokens):
        g = g_ref[t].astype(F32)
        o = o_ref[t].astype(F32)
        delta = jnp.sum(g * o, axis=-1, keepdims=True)
        norm_row = jnp.broadcast_to(n_ref[t : t + 1, :], (heads, heads))
        norm = jnp.sum(jnp.where(pick, norm_row, 0.0), axis=-1, keepdims=True) * root
        for p, part in enumerate(split_parts(norm) + split_parts(delta)):
            extra = jnp.where(lane == t * stride + p, part.astype(F32), extra)
    extra = extra.astype(BF)
    for k in range(kvs):
        head = kvs - 1 - k
        part = slice(head * group, (head + 1) * group)
        for t in range(tokens):
            m_ref[k, t * group : (t + 1) * group, :] = q_ref[t, part, :]
            m_ref[k, block + t * group : block + (t + 1) * group, :] = g_ref[t, part, :]
        m_ref[k, 2 * block : rows, :] = extra[part, :]
    stores = [pltpu.make_async_copy(m_ref, out_hbm.at[s], out_sems.at[s]) for s in range(seqs)]
    for store in stores:
        store.start()
    for store in stores:
        store.wait()


def unpack(m_ref, first, count, tokens, group):
    block = tokens * group
    stride = LANES // tokens
    q = m_ref[pl.ds(first, count), 0:block, :].reshape(count * block, LANES)
    g = m_ref[pl.ds(first, count), block : 2 * block, :].reshape(count * block, LANES)
    e = m_ref[pl.ds(first, count), 2 * block : 2 * block + group, :]
    lane = lax.broadcasted_iota(jnp.int32, (count, group, LANES), 2)
    pieces = [jnp.where((lane >= t * stride) & (lane < (t + 1) * stride), e, jnp.zeros_like(e)) for t in range(tokens)]
    extra = jnp.stack(pieces, axis=1).reshape(count * block, LANES)
    return q, g, extra


def stage_body(k_ref, v_ref, starts_ref, k_out, v_out, lo_ref, hi_ref, *, tokens, chips, cores, kvs):
    keys = k_ref.shape[0]
    stride = LANES // tokens
    row = lax.broadcasted_iota(jnp.int32, (LANES, keys), 0) % stride
    minus = jnp.full((LANES, keys), -1.0, F32)
    k_out[0:LANES, :] = k_ref[...].T
    k_out[LANES:, :] = jnp.where(row < PARTS, minus, 0.0).astype(BF)
    v_out[0:LANES, :] = v_ref[...].T
    v_out[LANES:, :] = jnp.where((row >= PARTS) & (row < 2 * PARTS), minus, 0.0).astype(BF)
    core = lax.axis_index("core")
    base = (lax.axis_index("chip") * cores + core) * keys
    each = kvs * tokens
    offset = chips * cores * (keys - each) - base

    def bounds(chip):
        for c in range(cores):
            first = (chip * cores + lax.rem(core + c, cores)) * each
            for i in range(each):
                row = pl.ds(chip * each + i, 1)
                t = first + (kvs - 1 - i // tokens) * tokens + i % tokens
                lo_ref[c, row, :] = jnp.full((1, LANES), starts_ref[t] - base, jnp.int32)
                hi_ref[c, row, :] = jnp.full((1, LANES), offset + t, jnp.int32)

    if chips <= 4:
        for chip in range(chips):
            bounds(chip)
    else:
        pl.loop(0, chips)(bounds)


def visible_bounds(ref, turn, first, count, group, span):
    each = [jnp.broadcast_to(ref[turn, pl.ds(first + t, 1), :], (group, LANES)) for t in range(count)]
    return jnp.tile(jnp.concatenate(each, axis=0), (1, span // LANES))


def scored(q_wide, g_wide, k_ref, v_ref, part, lo, hi, factor):
    scores = jnp.dot(q_wide, k_ref[:, part], preferred_element_type=F32)
    pulled = jnp.dot(g_wide, v_ref[:, part], preferred_element_type=F32)
    pos = lax.broadcasted_iota(jnp.int32, scores.shape, 1) + part.start
    weights = jnp.where((pos >= lo) & (pos <= hi), jnp.exp2(scores * factor), 0.0)
    return weights, weights * pulled


def grads_body(m_ref, key_ref, k_ref, v_ref, lo_ref, hi_ref, *rest, tokens, group, step, span, scaling, turn, last):
    if last:
        done, (dq_hbm, dq_ref, sems) = rest[:-3], rest[-3:]
    else:
        done, (dq_ref,) = rest[:-1], rest[-1:]
    messages = m_ref.shape[0]
    keys = key_ref.shape[0]
    block = tokens * group
    factor = scaling * math.log2(math.e)
    here = step * tokens
    if last:
        cores = dq_hbm.shape[1]
        core = lax.axis_index("core")

        def store(c, src):
            return pltpu.make_async_copy(src, dq_hbm.at[:, lax.rem(core + c, cores)], sems.at[c])

        for c, ref in enumerate(done):
            store(c, ref).start()

    def visit(at):
        q, g, extra = unpack(m_ref, at * step, step, tokens, group)
        q_wide = jnp.concatenate([q, extra], axis=1)
        g_wide = jnp.concatenate([g, extra], axis=1)
        lo = visible_bounds(lo_ref, turn, at * here, here, group, span)
        hi = visible_bounds(hi_ref, turn, at * here, here, group, span)
        dq = None
        for j in range(keys // span):
            part = slice(j * span, (j + 1) * span)
            _, s = scored(q_wide, g_wide, k_ref, v_ref, part, lo, hi, factor)
            add = jnp.dot(s.astype(BF), key_ref[part, :], preferred_element_type=F32)
            dq = add if dq is None else dq + add
        dq = (dq * scaling).astype(BF).reshape(step, block, LANES)
        kvs = dq_ref.shape[1]
        for i in range(step):
            dq_ref[(at * step + i) // kvs, (at * step + i) % kvs] = dq[i]

    steps = messages // step
    if steps <= 4:
        for at in range(steps):
            visit(at)
    else:
        pl.loop(0, steps)(visit)
    if last:
        store(turn, dq_ref).start()
        for c in range(turn):
            store(c, done[c]).wait()
        store(turn, dq_ref).wait()


def context_body(k_ref, v_ref, lo_ref, hi_ref, *refs, tokens, group, step, scaling):
    dk_ref, dv_ref = refs[-2:]
    block = tokens * group
    tn = (((0,), (0,)), ((), ()))
    keys = dk_ref.shape[0]
    factor = scaling * math.log2(math.e)
    here = step * tokens
    whole = slice(0, keys)
    sums = None
    for turn, m_ref in enumerate(refs[:-2]):

        def visit(at):
            q, g, extra = unpack(m_ref, at * step, step, tokens, group)
            lo = visible_bounds(lo_ref, turn, at * here, here, group, keys)
            hi = visible_bounds(hi_ref, turn, at * here, here, group, keys)
            q_wide = jnp.concatenate([q, extra], axis=1)
            g_wide = jnp.concatenate([g, extra], axis=1)
            w, s = scored(q_wide, g_wide, k_ref, v_ref, whole, lo, hi, factor)
            dk = lax.dot_general(s.astype(BF), q, tn, preferred_element_type=F32)
            dv = lax.dot_general(w.astype(BF), g, tn, preferred_element_type=F32)
            return dk, dv

        def add(at, sums):
            return tuple(old + new for old, new in zip(sums, visit(at), strict=True))

        steps = m_ref.shape[0] // step
        sums = visit(0) if sums is None else add(0, sums)
        if steps > 1:
            sums = lax.fori_loop(1, steps, add, sums)
    dk_ref[...] = (sums[0] * scaling).astype(BF)
    dv_ref[...] = sums[1].astype(BF)


def exchange(value, axes):
    outer = math.prod(lax.axis_size(a) for a in axes[:-1])
    inner = lax.axis_size(axes[-1])
    order = [o * inner + i for o in range(outer) for i in reversed(range(inner))]
    return lax.all_to_all(value, axes, split_axis=0, concat_axis=0, axis_index_groups=[order], tiled=True)


def combine_body(b_ref, dq_ref):
    seqs, kvs, tokens, group, _ = b_ref.shape
    for k in range(kvs):
        for t in range(tokens):
            total = b_ref[0, k, t].astype(F32)
            for s in range(1, seqs):
                total = total + b_ref[s, k, t].astype(F32)
            head = kvs - 1 - k
            dq_ref[t, head * group : (head + 1) * group, :] = total.astype(BF)


def local(queries, attn_out, grad_out, log_norms, query_starts, keys, values):
    scaling = queries.shape[-1] ** (-0.5)
    chips, cores, kvs = lax.axis_size("chip"), lax.axis_size("core"), lax.axis_size("kvh")
    senders = chips * kvs
    peers = senders * cores
    tokens, heads, width = queries.shape
    group = heads // kvs
    block = tokens * group
    slow = lambda value: pltpu.with_memory_space_constraint(value, pltpu.HBM)
    rows_sent = 2 * block + group
    message = kernel(
        functools.partial(prep_body, root=1.0 / scaling),
        8,
        out_shape=pltpu.HBM((chips, kvs, rows_sent, width), BF),
        in_specs=[ANY] * 4,
        out_specs=ANY,
        scratch_shapes=[
            pltpu.VMEM(queries.shape, BF),
            pltpu.VMEM(queries.shape, BF),
            pltpu.VMEM(queries.shape, BF),
            pltpu.VMEM(log_norms.shape, F32),
            pltpu.VMEM((kvs, rows_sent, width), BF),
            pltpu.SemaphoreType.DMA((4,)),
            pltpu.SemaphoreType.DMA((chips,)),
        ],
        name="prep",
    )(slow(queries), slow(grad_out), slow(attn_out), slow(log_norms))
    message = message.reshape(senders, rows_sent, width)
    own = exchange(message, ("chip", "kvh"))
    key_count = keys.shape[0]
    key_rows = fast(keys[:, 0, :])
    here = senders * tokens
    k_wide, v_wide, lo, hi = kernel(
        functools.partial(stage_body, tokens=tokens, chips=chips, cores=cores, kvs=kvs),
        8,
        out_shape=(
            held((2 * LANES, key_count)),
            held((2 * LANES, key_count)),
            held((cores, here, LANES), jnp.int32),
            held((cores, here, LANES), jnp.int32),
        ),
        in_specs=[VM, VM, pl.BlockSpec(memory_space=pltpu.SMEM)],
        out_specs=(VM,) * 4,
        name="stage",
    )(key_rows, values[:, 0, :], slow(query_starts))
    own, k_wide, v_wide, lo, hi = lax.optimization_barrier((own, k_wide, v_wide, lo, hi))
    got = [own]
    for c in range(1, cores):
        got.append(lax.ppermute(own, "core", [((i + c) % cores, i) for i in range(cores)]))
    step = math.gcd(senders, STEP)
    partials = []
    staged = (fast(k_wide), fast(v_wide), fast(lo), fast(hi))
    for turn in range(cores):
        last = turn == cores - 1
        scratch = [pltpu.VMEM((chips, kvs, block, width), BF), pltpu.SemaphoreType.DMA((cores,))]
        partial = kernel(
            functools.partial(
                grads_body,
                tokens=tokens,
                group=group,
                step=step,
                span=math.gcd(key_count, SPAN),
                scaling=scaling,
                turn=turn,
                last=last,
            ),
            40,
            out_shape=pltpu.HBM((chips, cores, kvs, block, width), BF) if last else held((chips, kvs, block, width)),
            in_specs=[VM] * (6 + turn),
            out_specs=ANY if last else VM,
            scratch_shapes=scratch if last else [],
            name=f"grads{turn}",
        )(fast(got[turn]), fast(key_rows), *staged, *map(fast, partials))
        partials.append(partial)
    partial = partials[-1].reshape(peers, block, width)
    back = exchange(partial, ("chip", "core", "kvh"))
    grad_keys, grad_values = kernel(
        functools.partial(context_body, tokens=tokens, group=group, step=step, scaling=scaling),
        40,
        out_shape=(jax.ShapeDtypeStruct((key_count, width), BF),) * 2,
        in_specs=[VM] * (4 + cores),
        out_specs=(VM, VM),
        name="context",
    )(*staged, *map(fast, got))
    grad_query = kernel(
        combine_body,
        8,
        out_shape=jax.ShapeDtypeStruct((tokens, heads, width), BF),
        in_specs=[VM],
        out_specs=VM,
        name="combine",
    )(fast(back.reshape(chips * cores, kvs, tokens, group, width)))
    return (grad_query, grad_keys[:, None, :], grad_values[:, None, :])


def solution(mesh):
    seqs, kvs = mesh.shape["seq"], mesh.shape["kvh"]
    cores = 2 if seqs % 2 == 0 else 1
    split = jax.sharding.Mesh(mesh.devices.reshape(seqs // cores, cores, kvs), ("chip", "core", "kvh"))
    token, context = ("chip", "core", "kvh"), ("chip", "core")
    return jax.shard_map(
        local,
        mesh=split,
        in_specs=(
            P(token, None, None),
            P(token, None, None),
            P(token, None, None),
            P(token, None),
            P(),
            P(context, "kvh", None),
            P(context, "kvh", None),
        ),
        out_specs=(P(token, None, None), P(context, "kvh", None), P(context, "kvh", None)),
        check_vma=False,
    )
```
